32 devices in a mesh: tm: 8 (over z, core), member: 4 (over y, x).
Axes of the slice: x: 2, y: 2, z: 4, core: 2. Of those that a mesh axis runs over, the one named last changes fastest.
Arguments:
- fields: float32 [48, 48, 8192], P('member', 'tm'), may hold values from 200 to 350, as said below
Outputs:
- covariance: float32 [48, 48, 8192], P('member', None, 'tm')
The draws below stay inside these ranges and needn't reach their ends.
Inputs may be any that keep to these rules, and one draw needn't show every extreme that they name: `fields`: month t is calendar month t mod 12.
All inputs are finite; a program needn't handle non-finite values.
Results may differ from the reference program's by a relative error of at most 0.0003.
Values sent between devices are 32-bit elements; how exact they have to be, the bound alone decides.
A program may use at most 192 MiB of HBM per device.

```python
import math
import jax
import jax.numpy as jnp
from jax import lax

MEMBERS = 48
MONTHS = 48
PIXELS = 8192


def draw_fields(key, part):
    subkeys = jax.random.split(key, 7)
    offset = jax.random.uniform(subkeys[0], (1, 1, PIXELS), jnp.float32, 250.0, 300.0)
    amplitude = jnp.exp(jax.random.uniform(subkeys[1], (1, 1, PIXELS), jnp.float32, 0.0, math.log(20.0)))
    phase_shift = jax.random.uniform(subkeys[2], (1, 1, PIXELS), jnp.float32, 0.0, 12.0)
    pixel_scale = jnp.exp(jax.random.uniform(subkeys[3], (1, 1, PIXELS), jnp.float32, math.log(0.3), math.log(3.0)))
    weight = jax.random.uniform(subkeys[4], (1, 1, PIXELS), jnp.float32, 0.6, 1.2)
    calendar = (jnp.arange(MONTHS) % 12).astype(jnp.float32).reshape(1, MONTHS, 1)
    season = amplitude * jnp.sin(2.0 * math.pi * (calendar + phase_shift) / 12.0)
    common = jax.random.normal(subkeys[5], (1, MONTHS, PIXELS), jnp.float32)
    member_noise = jax.random.normal(subkeys[6], (MEMBERS, MONTHS, PIXELS), jnp.float32)
    member_scale = jnp.ones((MEMBERS, 1, 1), jnp.float32)
    values = offset + season + pixel_scale * member_scale * (weight * common + member_noise)
    return jnp.clip(values, 200.0, 350.0).astype(jnp.float32)


def setup_inputs(seed: int = 0) -> dict:
    keys = jax.random.split(jax.random.key(seed), 2)
    return {
        "fields": draw_fields(jax.random.fold_in(keys[1], 71), 0),
    }


def monthly_anomaly(series):
    members_here, months_here, pixel_count = series.shape
    by_year = series.reshape(members_here, months_here // 12, 12, pixel_count)
    climatology = jnp.mean(by_year, axis=1, keepdims=True)
    return (by_year - climatology).reshape(members_here, months_here, pixel_count)


def reference(fields):
    anomaly = monthly_anomaly(fields)
    products = jnp.einsum("itp,jtp->ijp", anomaly, anomaly, precision=lax.Precision.HIGHEST, preferred_element_type=jnp.float32)
    return products / (MONTHS - 12)
```

```python
import functools
import math

import jax
import jax.numpy as jnp
from jax import lax
from jax.experimental import pallas as pl
from jax.experimental.pallas import tpu as pltpu
from jax.sharding import PartitionSpec as P

MESH = pl.DeviceIdType.MESH
LANES = 128
YEAR = 12


def contrasts(series, divisor):
    count = len(series)
    if count & (count - 1):
        mean = sum(series[1:], series[0]) * (1.0 / count)
        return [(s - mean) * (1.0 / math.sqrt(divisor)) for s in series]
    found, width = [], 1
    while len(series) > 1:
        width *= 2
        scale = 1.0 / math.sqrt(width * divisor)
        found += [(p - q) * scale for p, q in zip(series[::2], series[1::2])]
        series = [p + q for p, q in zip(series[::2], series[1::2])]
    return found


def kernel(dims, x_ref, out_ref, packed, landed, every, rows_of, cov, fsend, frecv, csend, crecv, own_sem):
    tms, groups, chunks, members, months, years = dims
    devices = tms * groups
    parts = YEAR // months
    terms = rows_of.shape[1]
    total = every.shape[1]
    a, b = lax.axis_index("tm"), lax.axis_index("member")
    me = a * groups + b

    def device(index):
        return (index // groups, lax.rem(index, groups))

    barrier = pltpu.get_barrier_semaphore()

    def greet(d, _):
        pl.semaphore_signal(
            barrier, inc=1, device_id=device(lax.rem(me + d, devices)), device_id_type=MESH
        )
        return 0

    lax.fori_loop(1, devices, greet, 0)

    def field_copy(k, source, dest, target):
        return pltpu.make_async_remote_copy(
            src_ref=packed.at[k, dest],
            dst_ref=landed.at[k, source],
            send_sem=fsend.at[k, dest],
            recv_sem=frecv.at[k, source],
            device_id=device(target),
            device_id_type=MESH,
        )

    def pack(dest, _):
        for k in range(chunks):
            columns = pl.ds(pl.multiple_of((dest * chunks + k) * LANES, LANES), LANES)
            for m in range(members):
                packed[k, dest, pl.ds(m, months, stride=members), :] = x_ref[m, :, columns]
        return 0

    lax.fori_loop(0, devices, pack, 0)
    pl.semaphore_wait(barrier, devices - 1)

    for k in range(chunks):

        def send(d, _):
            dest = lax.rem(me + d, devices)
            field_copy(k, me, dest, dest).start()
            return 0

        half = devices // 2
        lax.fori_loop(half, devices, send, 0)
        lax.fori_loop(1, half, send, 0)
        landed[k, me] = packed[k, me]

    def cov_copy(k, offset):
        return pltpu.make_async_remote_copy(
            src_ref=cov.at[k, offset],
            dst_ref=out_ref.at[:, :, pl.ds(pl.multiple_of((b * chunks + k) * LANES, LANES), LANES)],
            send_sem=csend.at[k, offset],
            recv_sem=crecv.at[k, offset],
            device_id=(a, lax.rem(b + offset, groups)),
            device_id_type=MESH,
        )

    def own_copy(k):
        return pltpu.make_async_copy(
            cov.at[k, 0],
            out_ref.at[:, :, pl.ds(pl.multiple_of((b * chunks + k) * LANES, LANES), LANES)],
            own_sem.at[k],
        )

    for k in range(chunks):

        def arrive(d, _):
            source = lax.rem(me + d, devices)
            field_copy(k, source, source, source).wait_recv()
            return 0

        lax.fori_loop(1, devices, arrive, 0)

        for part in range(parts):
            for g in range(groups):
                for c in range(months):
                    series = [
                        landed[k, (y * parts + part) * groups + g, c * members : (c + 1) * members, :]
                        for y in range(years)
                    ]
                    for q, u in enumerate(contrasts(series, float(years * YEAR - YEAR))):
                        t = (q * parts + part) * months + c
                        every[t, g * members : (g + 1) * members, :] = u
                        rows_of[g, t] = u

        for offset in list(range(1, groups)) + [0]:
            target = lax.rem(b + offset, groups)
            for first in range(0, total, 16):
                tiles = range(first, min(first + 16, total), 8)

                def step(t, sums):
                    across = [every[t, j : j + 8, :] for j in tiles]
                    new = []
                    for i in range(members):
                        row = jnp.broadcast_to(rows_of[target, t, i : i + 1, :], (8, LANES))
                        for n, v in enumerate(across):
                            new.append(sums[i * len(across) + n] + row * v)
                    return tuple(new)

                zero = jnp.zeros((8, LANES), jnp.float32)
                sums = lax.fori_loop(0, terms, step, (zero,) * (members * len(tiles)), unroll=2)
                for i in range(members):
                    for n, j in enumerate(tiles):
                        cov[k, offset, i, j : j + 8, :] = sums[i * len(tiles) + n]
            if offset:
                cov_copy(k, offset).start()
            else:
                own_copy(k).start()

    for k in range(chunks):

        def sent(d, _):
            dest = lax.rem(me + d, devices)
            field_copy(k, me, dest, dest).wait_send()
            return 0

        lax.fori_loop(1, devices, sent, 0)
        own_copy(k).wait()
        for offset in range(1, groups):
            cov_copy(k, offset).wait()


def solution(mesh):
    tms, groups = mesh.shape["tm"], mesh.shape["member"]

    def per_device(fields):
        members, months, pixels = fields.shape
        devices = tms * groups
        chunks = pixels // (devices * LANES)
        years = months * tms // YEAR
        terms = (years if years & (years - 1) else years - 1) * YEAR
        total = members * groups
        here = pixels // tms
        dims = (tms, groups, chunks, members, months, years)
        rows = members * months
        return pl.pallas_call(
            functools.partial(kernel, dims),
            out_shape=jax.ShapeDtypeStruct((members, total, here), jnp.float32),
            in_specs=[pl.BlockSpec(memory_space=pltpu.VMEM)],
            out_specs=pl.BlockSpec(memory_space=pl.ANY),
            scratch_shapes=[
                pltpu.VMEM((chunks, devices, rows, LANES), jnp.float32),
                pltpu.VMEM((chunks, devices, rows, LANES), jnp.float32),
                pltpu.VMEM((terms, total, LANES), jnp.float32),
                pltpu.VMEM((groups, terms, members, LANES), jnp.float32),
                pltpu.VMEM((chunks, groups, members, total, LANES), jnp.float32),
                pltpu.SemaphoreType.DMA((chunks, devices)),
                pltpu.SemaphoreType.DMA((chunks, devices)),
                pltpu.SemaphoreType.DMA((chunks, groups)),
                pltpu.SemaphoreType.DMA((chunks, groups)),
                pltpu.SemaphoreType.DMA((chunks,)),
            ],
            compiler_params=pltpu.CompilerParams(
                collective_id=0, has_side_effects=True, vmem_limit_bytes=48 * 1024 * 1024
            ),
        )(fields)

    return jax.shard_map(
        per_device,
        mesh=mesh,
        in_specs=(P("member", "tm", None),),
        out_specs=P("member", None, "tm"),
        check_vma=False,
    )
```

```python
import functools
import math

import jax
import jax.numpy as jnp
from jax import lax
from jax.experimental import pallas as pl
from jax.experimental.pallas import tpu as pltpu
from jax.sharding import PartitionSpec as P

MESH = pl.DeviceIdType.MESH
LANES = 128
YEAR = 12


def contrasts(series, divisor):
    count = len(series)
    if count & (count - 1):
        mean = sum(series[1:], series[0]) * (1.0 / count)
        return [(s - mean) * (1.0 / math.sqrt(divisor)) for s in series]
    found, width = [], 1
    while len(series) > 1:
        width *= 2
        scale = 1.0 / math.sqrt(width * divisor)
        found += [(p - q) * scale for p, q in zip(series[::2], series[1::2])]
        series = [p + q for p, q in zip(series[::2], series[1::2])]
    return found


def kernel(
    dims, x_hbm, out_ref, x_ref, packed, landed, every, rows_of, cov, halves, halves_in,
    xsem, fsend, frecv, csend, crecv,
):
    tms, groups, chunks, members, months, years, folded = dims
    devices = tms * groups
    parts = YEAR // months
    terms = rows_of.shape[1]
    total = every.shape[1]
    rows = members * months
    split = -(-rows // 16) * 8
    here = out_ref.shape[2]
    a, b = lax.axis_index("tm"), lax.axis_index("member")
    me = a * groups + b
    low = lax.broadcasted_iota(jnp.int32, (8, LANES), 1) < LANES // 2
    stages = [(k, None, 0, rows) for k in range(chunks)]
    if folded:
        stages[-1:] = [(chunks - 1, 0, 0, split), (chunks - 1, 1, split, rows)]

    def device(index):
        return (index // groups, lax.rem(index, groups))

    def piece(block):
        pixels = pl.ds(pl.multiple_of(block * here, LANES), here)
        return pltpu.make_async_copy(x_hbm.at[:, :, pixels], x_ref.at[:, :, pixels], xsem.at[block])

    def load(n, _):
        piece(lax.rem(a + tms // 2 + n, tms)).start()
        return 0

    lax.fori_loop(0, tms, load, 0)
    barrier = pltpu.get_barrier_semaphore()

    def greet(d, _):
        pl.semaphore_signal(
            barrier, inc=1, device_id=device(lax.rem(me + d, devices)), device_id_type=MESH
        )
        return 0

    lax.fori_loop(1, devices, greet, 0)

    def field_copy(s, source, dest):
        k, _, first, last = stages[s]
        return pltpu.make_async_remote_copy(
            src_ref=packed.at[k, dest, pl.ds(first, last - first)],
            dst_ref=landed.at[k, source, pl.ds(first, last - first)],
            send_sem=fsend.at[s, dest],
            recv_sem=frecv.at[s, source],
            device_id=device(dest),
            device_id_type=MESH,
        )

    def swap(v):
        return pltpu.roll(v, LANES // 2, 1)

    def pack(k, half, dest):
        columns = pl.ds(pl.multiple_of((dest * chunks + k) * LANES, LANES), LANES)
        for m in range(members):
            if half is None:
                packed[k, dest, pl.ds(m, months, stride=members), :] = x_ref[m, :, columns]
            else:
                cut = months // 2
                p, q = x_ref[m, :cut, columns], x_ref[m, cut:, columns]
                mask = lax.broadcasted_iota(jnp.int32, p.shape, 1) < LANES // 2
                packed[k, dest, pl.ds(m, cut, stride=members), :] = jnp.where(mask, p, swap(q))
                packed[k, dest, pl.ds(rows // 2 + m, cut, stride=members), :] = jnp.where(mask, swap(p), q)

    for s, (k, half, _, _) in enumerate(stages):

        def block(n, _):
            to = lax.rem(a + tms // 2 + n, tms)
            if s == 0:
                piece(to).wait()
            if not half:

                def pack_one(g, _):
                    pack(k, half, to * groups + g)
                    return 0

                lax.fori_loop(0, groups, pack_one, 0)
            if s == 0:

                @pl.when(n == 0)
                def _():
                    pl.semaphore_wait(barrier, devices - 1)

            def send(g, _):
                dest = to * groups + lax.rem(b + g, groups)

                @pl.when(dest != me)
                def _():
                    field_copy(s, me, dest).start()

                return 0

            lax.fori_loop(0, groups, send, 0)
            return 0

        lax.fori_loop(0, tms, block, 0)
    for k in range(chunks):
        landed[k, me] = packed[k, me]

    def columns_of(k, group):
        return pl.ds(pl.multiple_of((group * chunks + k) * LANES, LANES), LANES)

    def cov_copy(s, offset):
        k, half, _, _ = stages[s]
        return pltpu.make_async_remote_copy(
            src_ref=cov.at[k, offset - 1] if half is None else halves.at[half, offset],
            dst_ref=out_ref.at[:, :, columns_of(k, b)] if half is None else halves_in.at[half, offset],
            send_sem=csend.at[s, offset],
            recv_sem=crecv.at[s, offset],
            device_id=(a, lax.rem(b + offset, groups)),
            device_id_type=MESH,
        )

    for s, (k, half, _, _) in enumerate(stages):

        def arrive(d, _):
            source = lax.rem(me + d, devices)
            field_copy(s, source, source).wait_recv()
            return 0

        lax.fori_loop(1, devices, arrive, 0)
        spans = months if half is None else months // 2
        base = rows // 2 if half else 0
        for part in range(parts):
            for g in range(groups):
                for c in range(spans):
                    at = base + c * members
                    series = [
                        landed[k, (y * parts + part) * groups + g, at : at + members, :]
                        for y in range(years)
                    ]
                    for q, u in enumerate(contrasts(series, float(years * YEAR - YEAR))):
                        t = (q * parts + part) * spans + c
                        every[t, g * members : (g + 1) * members, :] = u
                        rows_of[g, t] = u

        for offset in list(range(1, groups)) + [0]:
            target = lax.rem(b + offset, groups)
            for first in range(0, total, 16):
                tiles = range(first, min(first + 16, total), 8)

                def step(t, sums):
                    across = [every[t, j : j + 8, :] for j in tiles]
                    new = []
                    for i in range(members):
                        row = jnp.broadcast_to(rows_of[target, t, i : i + 1, :], (8, LANES))
                        for n, v in enumerate(across):
                            new.append(sums[i * len(across) + n] + row * v)
                    return tuple(new)

                zero = jnp.zeros((8, LANES), jnp.float32)
                used = terms if half is None else terms // 2
                sums = lax.fori_loop(0, used, step, (zero,) * (members * len(tiles)), unroll=2)
                for n, j in enumerate(tiles):
                    got = sums[n :: len(tiles)]
                    if half is not None:
                        for p in range(members // 2):
                            u, v = got[2 * p + half], got[2 * p + 1 - half]
                            halves[half, offset, p, j : j + 8, :] = jnp.where(low, u, v) + swap(
                                jnp.where(low, v, u)
                            )
                    elif offset:
                        for i in range(members):
                            cov[k, offset - 1, i, j : j + 8, :] = got[i]
                    else:
                        for i in range(members):
                            out_ref[i, j : j + 8, columns_of(k, b)] = got[i]
            if offset:
                cov_copy(s, offset).start()

    if folded:
        s, k = len(stages) - 1, chunks - 1
        for offset in range(groups):
            for half in range(2):
                if offset:
                    cov_copy(s - 1 + half, offset).wait_recv()
            here_in = halves_in if offset else halves
            columns = columns_of(k, lax.rem(b + groups - offset, groups))

            def unpack(p, _):
                for j in range(0, total, 8):
                    u, v = here_in[0, offset, p, j : j + 8, :], here_in[1, offset, p, j : j + 8, :]
                    out_ref[2 * p, j : j + 8, columns] = jnp.where(low, u, v)
                    out_ref[2 * p + 1, j : j + 8, columns] = swap(jnp.where(low, v, u))
                return 0

            lax.fori_loop(0, members // 2, unpack, 0)

    for s, (k, half, _, _) in enumerate(stages):

        def sent(d, _):
            field_copy(s, me, lax.rem(me + d, devices)).wait_send()
            return 0

        lax.fori_loop(1, devices, sent, 0)
        for offset in range(1, groups):
            if half is None:
                cov_copy(s, offset).wait_recv()
            cov_copy(s, offset).wait_send()


def solution(mesh):
    tms, groups = mesh.shape["tm"], mesh.shape["member"]

    def per_device(fields):
        members, months, pixels = fields.shape
        devices = tms * groups
        chunks = pixels // (devices * LANES)
        years = months * tms // YEAR
        terms = (years if years & (years - 1) else years - 1) * YEAR
        total = members * groups
        here = pixels // tms
        rows = members * months
        folded = rows % 8 == 0 and months % 2 == 0 and members % 2 == 0
        dims = (tms, groups, chunks, members, months, years, folded)
        stages = chunks + folded
        pairs = members // 2 if folded else 1
        return pl.pallas_call(
            functools.partial(kernel, dims),
            out_shape=jax.ShapeDtypeStruct((members, total, here), jnp.float32),
            in_specs=[pl.BlockSpec(memory_space=pltpu.HBM)],
            out_specs=pl.BlockSpec(memory_space=pltpu.VMEM),
            scratch_shapes=[
                pltpu.VMEM((members, months, pixels), jnp.float32),
                pltpu.VMEM((chunks, devices, rows, LANES), jnp.float32),
                pltpu.VMEM((chunks, devices, rows, LANES), jnp.float32),
                pltpu.VMEM((terms, total, LANES), jnp.float32),
                pltpu.VMEM((groups, terms, members, LANES), jnp.float32),
                pltpu.VMEM((chunks, groups - 1, members, total, LANES), jnp.float32),
                pltpu.VMEM((2, groups, pairs, total, LANES), jnp.float32),
                pltpu.VMEM((2, groups, pairs, total, LANES), jnp.float32),
                pltpu.SemaphoreType.DMA((tms,)),
                pltpu.SemaphoreType.DMA((stages, devices)),
                pltpu.SemaphoreType.DMA((stages, devices)),
                pltpu.SemaphoreType.DMA((stages, groups)),
                pltpu.SemaphoreType.DMA((stages, groups)),
            ],
            compiler_params=pltpu.CompilerParams(
                collective_id=0, has_side_effects=True, vmem_limit_bytes=48 * 1024 * 1024
            ),
        )(fields)

    return jax.shard_map(
        per_device,
        mesh=mesh,
        in_specs=(P("member", "tm", None),),
        out_specs=P("member", None, "tm"),
        check_vma=False,
    )
```

```python
import functools
import math

import jax
import jax.numpy as jnp
from jax import lax
from jax.experimental import pallas as pl
from jax.experimental.pallas import tpu as pltpu
from jax.sharding import PartitionSpec as P

MESH = pl.DeviceIdType.MESH
LANES = 128
YEAR = 12


def contrasts(series, divisor):
    count = len(series)
    if count & (count - 1):
        mean = sum(series[1:], series[0]) * (1.0 / count)
        return [(s - mean) * (1.0 / math.sqrt(divisor)) for s in series]
    found, width = [], 1
    while len(series) > 1:
        width *= 2
        scale = 1.0 / math.sqrt(width * divisor)
        found += [(p - q) * scale for p, q in zip(series[::2], series[1::2])]
        series = [p + q for p, q in zip(series[::2], series[1::2])]
    return found


def kernel(
    dims, x_hbm, out_ref, x_ref, packed, landed, every, rows_of, cov, halves, halves_in,
    xsem, fsend, frecv, csend, crecv,
):
    tms, groups, chunks, members, months, years, folded = dims
    devices = tms * groups
    parts = YEAR // months
    terms = rows_of.shape[1]
    total = every.shape[1]
    rows = members * months
    split = -(-rows // 16) * 8
    here = out_ref.shape[2]
    a, b = lax.axis_index("tm"), lax.axis_index("member")
    me = a * groups + b
    low = lax.broadcasted_iota(jnp.int32, (8, LANES), 1) < LANES // 2
    stages = [(k, None, 0, rows) for k in range(chunks)]
    if folded:
        stages[-1:] = [(chunks - 1, 0, 0, split), (chunks - 1, 1, split, rows)]

    def device(index):
        return (index // groups, lax.rem(index, groups))

    def piece(block):
        pixels = pl.ds(pl.multiple_of(block * here, LANES), here)
        return pltpu.make_async_copy(x_hbm.at[:, :, pixels], x_ref.at[:, :, pixels], xsem.at[block])

    def load(n, _):
        piece(lax.rem(a + tms // 2 + n, tms)).start()
        return 0

    lax.fori_loop(0, tms, load, 0)
    barrier = pltpu.get_barrier_semaphore()

    def greet(d, _):
        pl.semaphore_signal(
            barrier, inc=1, device_id=device(lax.rem(me + d, devices)), device_id_type=MESH
        )
        return 0

    lax.fori_loop(1, devices, greet, 0)

    def field_copy(s, source, dest):
        k, _, first, last = stages[s]
        return pltpu.make_async_remote_copy(
            src_ref=packed.at[k, dest, pl.ds(first, last - first)],
            dst_ref=landed.at[k, source, pl.ds(first, last - first)],
            send_sem=fsend.at[s, dest],
            recv_sem=frecv.at[s, source],
            device_id=device(dest),
            device_id_type=MESH,
        )

    def swap(v):
        return pltpu.roll(v, LANES // 2, 1)

    def pack(k, half, dest):
        columns = pl.ds(pl.multiple_of((dest * chunks + k) * LANES, LANES), LANES)
        for m in range(members):
            if half is None:
                packed[k, dest, pl.ds(m, months, stride=members), :] = x_ref[m, :, columns]
            else:
                cut = months // 2
                p, q = x_ref[m, :cut, columns], x_ref[m, cut:, columns]
                mask = lax.broadcasted_iota(jnp.int32, p.shape, 1) < LANES // 2
                packed[k, dest, pl.ds(m, cut, stride=members), :] = jnp.where(mask, p, swap(q))
                packed[k, dest, pl.ds(rows // 2 + m, cut, stride=members), :] = jnp.where(mask, swap(p), q)

    def send_stage(s):
        k, half, _, _ = stages[s]

        def block(n, _):
            to = lax.rem(a + tms // 2 + n, tms)
            if s == 0:
                piece(to).wait()
            if not half:

                def pack_one(g, _):
                    pack(k, half, to * groups + g)
                    return 0

                lax.fori_loop(0, groups, pack_one, 0)
            if s == 0:

                @pl.when(n == 0)
                def _():
                    pl.semaphore_wait(barrier, devices - 1)

            def send(g, _):
                dest = to * groups + lax.rem(b + g + 1, groups)

                @pl.when(dest != me)
                def _():
                    field_copy(s, me, dest).start()

                return 0

            lax.fori_loop(0, groups, send, 0)
            return 0

        lax.fori_loop(0, tms, block, 0)

    early = min(2, len(stages))
    for s in range(early):
        send_stage(s)
    for k in range(chunks):
        landed[k, me] = packed[k, me]

    def columns_of(k, group):
        return pl.ds(pl.multiple_of((group * chunks + k) * LANES, LANES), LANES)

    def cov_copy(s, offset):
        k, half, _, _ = stages[s]
        return pltpu.make_async_remote_copy(
            src_ref=cov.at[k, offset - 1] if half is None else halves.at[half, offset],
            dst_ref=out_ref.at[:, :, columns_of(k, b)] if half is None else halves_in.at[half, offset],
            send_sem=csend.at[s, offset],
            recv_sem=crecv.at[s, offset],
            device_id=(a, lax.rem(b + offset, groups)),
            device_id_type=MESH,
        )

    for s, (k, half, _, _) in enumerate(stages):

        def arrive(d, _):
            source = lax.rem(me + d, devices)
            field_copy(s, source, source).wait_recv()
            return 0

        lax.fori_loop(1, devices, arrive, 0)
        spans = months if half is None else months // 2
        base = rows // 2 if half else 0
        for part in range(parts):
            for g in range(groups):
                for c in range(spans):
                    at = base + c * members
                    series = [
                        landed[k, (y * parts + part) * groups + g, at : at + members, :]
                        for y in range(years)
                    ]
                    for q, u in enumerate(contrasts(series, float(years * YEAR - YEAR))):
                        t = (q * parts + part) * spans + c
                        every[t, g * members : (g + 1) * members, :] = u
                        rows_of[g, t] = u

        for offset in list(range(1, groups)) + [0]:
            target = lax.rem(b + offset, groups)
            for first in range(0, total, 16):
                tiles = range(first, min(first + 16, total), 8)

                def step(t, sums):
                    across = [every[t, j : j + 8, :] for j in tiles]
                    new = []
                    for i in range(members):
                        row = jnp.broadcast_to(rows_of[target, t, i : i + 1, :], (8, LANES))
                        for n, v in enumerate(across):
                            new.append(sums[i * len(across) + n] + row * v)
                    return tuple(new)

                zero = jnp.zeros((8, LANES), jnp.float32)
                used = terms if half is None else terms // 2
                sums = lax.fori_loop(0, used, step, (zero,) * (members * len(tiles)), unroll=2)
                for n, j in enumerate(tiles):
                    got = sums[n :: len(tiles)]
                    if half is not None:
                        for p in range(members // 2):
                            u, v = got[2 * p + half], got[2 * p + 1 - half]
                            halves[half, offset, p, j : j + 8, :] = jnp.where(low, u, v) + swap(
                                jnp.where(low, v, u)
                            )
                    elif offset:
                        for i in range(members):
                            cov[k, offset - 1, i, j : j + 8, :] = got[i]
                    else:
                        for i in range(members):
                            out_ref[i, j : j + 8, columns_of(k, b)] = got[i]
            if offset:
                cov_copy(s, offset).start()
            if offset == groups - 1 and s == 0:
                for later in range(early, len(stages)):
                    send_stage(later)

    if folded:
        s, k = len(stages) - 1, chunks - 1
        for offset in range(groups):
            for half in range(2):
                if offset:
                    cov_copy(s - 1 + half, offset).wait_recv()
            here_in = halves_in if offset else halves
            columns = columns_of(k, lax.rem(b + groups - offset, groups))

            def unpack(p, _):
                for j in range(0, total, 8):
                    u, v = here_in[0, offset, p, j : j + 8, :], here_in[1, offset, p, j : j + 8, :]
                    out_ref[2 * p, j : j + 8, columns] = jnp.where(low, u, v)
                    out_ref[2 * p + 1, j : j + 8, columns] = swap(jnp.where(low, v, u))
                return 0

            lax.fori_loop(0, members // 2, unpack, 0)

    for s, (k, half, _, _) in enumerate(stages):

        def sent(d, _):
            field_copy(s, me, lax.rem(me + d, devices)).wait_send()
            return 0

        lax.fori_loop(1, devices, sent, 0)
        for offset in range(1, groups):
            if half is None:
                cov_copy(s, offset).wait_recv()
            cov_copy(s, offset).wait_send()


def solution(mesh):
    tms, groups = mesh.shape["tm"], mesh.shape["member"]

    def per_device(fields):
        members, months, pixels = fields.shape
        devices = tms * groups
        chunks = pixels // (devices * LANES)
        years = months * tms // YEAR
        terms = (years if years & (years - 1) else years - 1) * YEAR
        total = members * groups
        here = pixels // tms
        rows = members * months
        folded = rows % 8 == 0 and months % 2 == 0 and members % 2 == 0
        dims = (tms, groups, chunks, members, months, years, folded)
        stages = chunks + folded
        pairs = members // 2 if folded else 1
        return pl.pallas_call(
            functools.partial(kernel, dims),
            out_shape=jax.ShapeDtypeStruct((members, total, here), jnp.float32),
            in_specs=[pl.BlockSpec(memory_space=pltpu.HBM)],
            out_specs=pl.BlockSpec(memory_space=pltpu.VMEM),
            scratch_shapes=[
                pltpu.VMEM((members, months, pixels), jnp.float32),
                pltpu.VMEM((chunks, devices, rows, LANES), jnp.float32),
                pltpu.VMEM((chunks, devices, rows, LANES), jnp.float32),
                pltpu.VMEM((terms, total, LANES), jnp.float32),
                pltpu.VMEM((groups, terms, members, LANES), jnp.float32),
                pltpu.VMEM((chunks, groups - 1, members, total, LANES), jnp.float32),
                pltpu.VMEM((2, groups, pairs, total, LANES), jnp.float32),
                pltpu.VMEM((2, groups, pairs, total, LANES), jnp.float32),
                pltpu.SemaphoreType.DMA((tms,)),
                pltpu.SemaphoreType.DMA((stages, devices)),
                pltpu.SemaphoreType.DMA((stages, devices)),
                pltpu.SemaphoreType.DMA((stages, groups)),
                pltpu.SemaphoreType.DMA((stages, groups)),
            ],
            compiler_params=pltpu.CompilerParams(
                collective_id=0, has_side_effects=True, vmem_limit_bytes=48 * 1024 * 1024
            ),
        )(fields)

    return jax.shard_map(
        per_device,
        mesh=mesh,
        in_specs=(P("member", "tm", None),),
        out_specs=P("member", None, "tm"),
        check_vma=False,
    )
```

```python
import functools
import math

import jax
import jax.numpy as jnp
from jax import lax
from jax.experimental import pallas as pl
from jax.experimental.pallas import tpu as pltpu
from jax.sharding import PartitionSpec as P

MESH = pl.DeviceIdType.MESH
LANES = 128
YEAR = 12


def contrasts(series, divisor):
    count = len(series)
    if count & (count - 1):
        mean = sum(series[1:], series[0]) * (1.0 / count)
        return [(s - mean) * (1.0 / math.sqrt(divisor)) for s in series]
    found, width = [], 1
    while len(series) > 1:
        width *= 2
        scale = 1.0 / math.sqrt(width * divisor)
        found += [(p - q) * scale for p, q in zip(series[::2], series[1::2])]
        series = [p + q for p, q in zip(series[::2], series[1::2])]
    return found


def kernel(
    dims, x_hbm, out_ref, x_ref, packed, landed, every, rows_of, cov, halves, halves_in,
    xsem, fsend, frecv, csend, crecv,
):
    tms, groups, chunks, members, months, years, folded = dims
    devices = tms * groups
    parts = YEAR // months
    terms = rows_of.shape[1]
    total = every.shape[1]
    rows = members * months
    split = -(-rows // 16) * 8
    here = out_ref.shape[2]
    a, b = lax.axis_index("tm"), lax.axis_index("member")
    me = a * groups + b
    low = lax.broadcasted_iota(jnp.int32, (8, LANES), 1) < LANES // 2
    stages = [(k, None, 0, rows) for k in range(chunks)]
    if folded:
        stages[-1:] = [(chunks - 1, 0, 0, split), (chunks - 1, 1, split, rows)]

    def device(index):
        return (index // groups, lax.rem(index, groups))

    def piece(block):
        pixels = pl.ds(pl.multiple_of(block * here, LANES), here)
        return pltpu.make_async_copy(x_hbm.at[:, :, pixels], x_ref.at[:, :, pixels], xsem.at[block])

    def load(n, _):
        piece(lax.rem(a + tms // 2 + n, tms)).start()
        return 0

    lax.fori_loop(0, tms, load, 0)
    barrier = pltpu.get_barrier_semaphore()

    def greet(d, _):
        pl.semaphore_signal(
            barrier, inc=1, device_id=device(lax.rem(me + d, devices)), device_id_type=MESH
        )
        return 0

    lax.fori_loop(1, devices, greet, 0)

    def field_copy(s, source, dest):
        k, _, first, last = stages[s]
        return pltpu.make_async_remote_copy(
            src_ref=packed.at[k, dest, pl.ds(first, last - first)],
            dst_ref=landed.at[k, source, pl.ds(first, last - first)],
            send_sem=fsend.at[s, dest],
            recv_sem=frecv.at[s, source],
            device_id=device(dest),
            device_id_type=MESH,
        )

    def swap(v):
        return pltpu.roll(v, LANES // 2, 1)

    def pack(k, half, dest):
        columns = pl.ds(pl.multiple_of((dest * chunks + k) * LANES, LANES), LANES)
        for m in range(members):
            if half is None:
                packed[k, dest, pl.ds(m, months, stride=members), :] = x_ref[m, :, columns]
            else:
                cut = months // 2
                p, q = x_ref[m, :cut, columns], x_ref[m, cut:, columns]
                mask = lax.broadcasted_iota(jnp.int32, p.shape, 1) < LANES // 2
                packed[k, dest, pl.ds(m, cut, stride=members), :] = jnp.where(mask, p, swap(q))
                packed[k, dest, pl.ds(rows // 2 + m, cut, stride=members), :] = jnp.where(mask, swap(p), q)

    for s, (k, half, _, _) in enumerate(stages):

        def block(n, _):
            to = lax.rem(a + tms // 2 + n, tms)
            if s == 0:
                piece(to).wait()
            if not half:

                def pack_one(g, _):
                    pack(k, half, to * groups + g)
                    return 0

                lax.fori_loop(0, groups, pack_one, 0)
            if s == 0:

                @pl.when(n == 0)
                def _():
                    pl.semaphore_wait(barrier, devices - 1)

            def send(g, _):
                dest = to * groups + lax.rem(b + g + 1, groups)

                @pl.when(dest != me)
                def _():
                    field_copy(s, me, dest).start()

                return 0

            lax.fori_loop(0, groups, send, 0)
            return 0

        lax.fori_loop(0, tms, block, 0)
    for k in range(chunks):
        landed[k, me] = packed[k, me]

    def columns_of(k, group):
        return pl.ds(pl.multiple_of((group * chunks + k) * LANES, LANES), LANES)

    def cov_copy(s, offset):
        k, half, _, _ = stages[s]
        return pltpu.make_async_remote_copy(
            src_ref=cov.at[k, offset - 1] if half is None else halves.at[half, offset],
            dst_ref=out_ref.at[:, :, columns_of(k, b)] if half is None else halves_in.at[half, offset],
            send_sem=csend.at[s, offset],
            recv_sem=crecv.at[s, offset],
            device_id=(a, lax.rem(b + offset, groups)),
            device_id_type=MESH,
        )

    for s, (k, half, _, _) in enumerate(stages):

        def arrive(d, _):
            source = lax.rem(me + d, devices)
            field_copy(s, source, source).wait_recv()
            return 0

        lax.fori_loop(1, devices, arrive, 0)
        spans = months if half is None else months // 2
        base = rows // 2 if half else 0
        for part in range(parts):
            for g in range(groups):
                for c in range(spans):
                    at = base + c * members
                    series = [
                        landed[k, (y * parts + part) * groups + g, at : at + members, :]
                        for y in range(years)
                    ]
                    for q, u in enumerate(contrasts(series, float(years * YEAR - YEAR))):
                        t = (q * parts + part) * spans + c
                        every[t, g * members : (g + 1) * members, :] = u
                        rows_of[g, t] = u

        for offset in list(range(1, groups)) + [0]:
            target = lax.rem(b + offset, groups)
            for first in range(0, total, 16):
                tiles = range(first, min(first + 16, total), 8)

                def step(t, sums):
                    across = [every[t, j : j + 8, :] for j in tiles]
                    new = []
                    for i in range(members):
                        row = jnp.broadcast_to(rows_of[target, t, i : i + 1, :], (8, LANES))
                        for n, v in enumerate(across):
                            new.append(sums[i * len(across) + n] + row * v)
                    return tuple(new)

                zero = jnp.zeros((8, LANES), jnp.float32)
                used = terms if half is None else terms // 2
                sums = lax.fori_loop(0, used, step, (zero,) * (members * len(tiles)), unroll=2)
                for n, j in enumerate(tiles):
                    got = sums[n :: len(tiles)]
                    if half is not None:
                        for p in range(members // 2):
                            u, v = got[2 * p + half], got[2 * p + 1 - half]
                            halves[half, offset, p, j : j + 8, :] = jnp.where(low, u, v) + swap(
                                jnp.where(low, v, u)
                            )
                    elif offset:
                        for i in range(members):
                            cov[k, offset - 1, i, j : j + 8, :] = got[i]
                    else:
                        for i in range(members):
                            out_ref[i, j : j + 8, columns_of(k, b)] = got[i]
            if offset:
                cov_copy(s, offset).start()

    if folded:
        s, k = len(stages) - 1, chunks - 1
        for offset in range(groups):
            for half in range(2):
                if offset:
                    cov_copy(s - 1 + half, offset).wait_recv()
            here_in = halves_in if offset else halves
            columns = columns_of(k, lax.rem(b + groups - offset, groups))

            def unpack(p, _):
                for j in range(0, total, 8):
                    u, v = here_in[0, offset, p, j : j + 8, :], here_in[1, offset, p, j : j + 8, :]
                    out_ref[2 * p, j : j + 8, columns] = jnp.where(low, u, v)
                    out_ref[2 * p + 1, j : j + 8, columns] = swap(jnp.where(low, v, u))
                return 0

            lax.fori_loop(0, members // 2, unpack, 0)

    for s, (k, half, _, _) in enumerate(stages):

        def sent(d, _):
            field_copy(s, me, lax.rem(me + d, devices)).wait_send()
            return 0

        lax.fori_loop(1, devices, sent, 0)
        for offset in range(1, groups):
            if half is None:
                cov_copy(s, offset).wait_recv()
            cov_copy(s, offset).wait_send()


def solution(mesh):
    tms, groups = mesh.shape["tm"], mesh.shape["member"]

    def per_device(fields):
        members, months, pixels = fields.shape
        devices = tms * groups
        chunks = pixels // (devices * LANES)
        years = months * tms // YEAR
        terms = (years if years & (years - 1) else years - 1) * YEAR
        total = members * groups
        here = pixels // tms
        rows = members * months
        folded = rows % 8 == 0 and months % 2 == 0 and members % 2 == 0
        dims = (tms, groups, chunks, members, months, years, folded)
        stages = chunks + folded
        pairs = members // 2 if folded else 1
        return pl.pallas_call(
            functools.partial(kernel, dims),
            out_shape=jax.ShapeDtypeStruct((members, total, here), jnp.float32),
            in_specs=[pl.BlockSpec(memory_space=pltpu.HBM)],
            out_specs=pl.BlockSpec(memory_space=pltpu.VMEM),
            scratch_shapes=[
                pltpu.VMEM((members, months, pixels), jnp.float32),
                pltpu.VMEM((chunks, devices, rows, LANES), jnp.float32),
                pltpu.VMEM((chunks, devices, rows, LANES), jnp.float32),
                pltpu.VMEM((terms, total, LANES), jnp.float32),
                pltpu.VMEM((groups, terms, members, LANES), jnp.float32),
                pltpu.VMEM((chunks, groups - 1, members, total, LANES), jnp.float32),
                pltpu.VMEM((2, groups, pairs, total, LANES), jnp.float32),
                pltpu.VMEM((2, groups, pairs, total, LANES), jnp.float32),
                pltpu.SemaphoreType.DMA((tms,)),
                pltpu.SemaphoreType.DMA((stages, devices)),
                pltpu.SemaphoreType.DMA((stages, devices)),
                pltpu.SemaphoreType.DMA((stages, groups)),
                pltpu.SemaphoreType.DMA((stages, groups)),
            ],
            compiler_params=pltpu.CompilerParams(
                collective_id=0, has_side_effects=True, vmem_limit_bytes=48 * 1024 * 1024
            ),
        )(fields)

    return jax.shard_map(
        per_device,
        mesh=mesh,
        in_specs=(P("member", "tm", None),),
        out_specs=P("member", None, "tm"),
        check_vma=False,
    )
```
